16 devices in a mesh: tp: 2 (over z), cp: 2 (over y), dp: 4 (over x, core).
Axes of the slice: x: 2, y: 2, z: 2, core: 2. Of those that a mesh axis runs over, the one named last changes fastest.
Arguments:
- hidden: bfloat16 [64, 64, 2048], P('dp', 'cp')
- tokens: int32 [64, 64], P('dp', 'cp')
- seq_lens: int32 [64], P('dp')
- norm_gain: float32 [2048], replicated
- w_head: bfloat16 [2048, 49152], P(None, 'tp')
Outputs:
- output 1: float32 [64, 64], P('dp', 'cp')
- output 2: float32 [], replicated
- output 3: bfloat16 [64, 64, 2048], P('dp', 'cp')
- output 4: float32 [2048], replicated
- output 5: float32 [2048, 49152], P(None, 'tp')
All inputs are finite; a program needn't handle non-finite values.
Results may differ from the reference program's by a relative error of at most 0.001.
Values sent between devices are 32-bit elements.
A program may use at most 1.25 GiB of HBM per device.

```python
import jax
import jax.numpy as jnp
from jax import lax

HIDDEN = 2048
VOCAB_SIZE = 49152
BATCH_ALL = 64
SEQ_LEN = 64
CP_SIZE = 2
ROW_BLOCK = 16
SEG_SIZE = SEQ_LEN // (2 * CP_SIZE)
NORM_EPS = 1e-5


def setup_inputs(seed: int = 0) -> dict:
    key = jax.random.key(seed)
    k_hid, k_tok, k_len, k_gain, k_head = jax.random.split(key, 5)
    hidden = jax.random.normal(k_hid, (BATCH_ALL, SEQ_LEN, HIDDEN), jnp.float32).astype(jnp.bfloat16)
    tokens = jax.random.randint(k_tok, (BATCH_ALL, SEQ_LEN), 0, VOCAB_SIZE, jnp.int32)
    seq_lens = jax.random.randint(k_len, (BATCH_ALL,), SEQ_LEN // 2, SEQ_LEN + 1, jnp.int32).at[0].set(SEQ_LEN)
    norm_gain = 1.0 + 0.3 * jax.random.normal(k_gain, (HIDDEN,), jnp.float32)
    w_head = (2.0 * HIDDEN ** -0.5 * jax.random.normal(k_head, (HIDDEN, VOCAB_SIZE), jnp.float32)).astype(jnp.bfloat16)
    return {'hidden': hidden, 'tokens': tokens, 'seq_lens': seq_lens, 'norm_gain': norm_gain, 'w_head': w_head}


def layout_labels(tokens):
    n_seqs = tokens.shape[0]
    seg_grid = tokens.reshape(n_seqs, CP_SIZE, 2, SEG_SIZE)
    first_end = jnp.concatenate([seg_grid[:, 1:, 0, 0], seg_grid[:, CP_SIZE - 1:, 1, 0]], axis=1)
    second_end = jnp.concatenate([seg_grid[:, :1, 1, 0], seg_grid[:, :CP_SIZE - 1, 1, 0]], axis=1)
    ends = jnp.stack([first_end, second_end], axis=2)
    labels = jnp.concatenate([seg_grid[..., 1:], ends[..., None]], axis=3)
    return labels.reshape(n_seqs, SEQ_LEN)


def layout_positions():
    rank_ids = jnp.arange(CP_SIZE)
    seg_ids = jnp.stack([rank_ids, 2 * CP_SIZE - 1 - rank_ids], axis=1)
    return (seg_ids[:, :, None] * SEG_SIZE + jnp.arange(SEG_SIZE)).reshape(SEQ_LEN)


def reference(hidden, tokens, seq_lens, norm_gain, w_head):
    labels = layout_labels(tokens)
    positions = layout_positions()
    valid_mask = (positions[None, :] + 1 < seq_lens[:, None]).astype(jnp.float32)
    valid_count = jnp.sum(seq_lens - 1).astype(jnp.float32)
    n_blocks = BATCH_ALL * SEQ_LEN // ROW_BLOCK
    rows_h = hidden.reshape(n_blocks, ROW_BLOCK, HIDDEN)
    rows_lab = labels.reshape(n_blocks, ROW_BLOCK)
    rows_valid = valid_mask.reshape(n_blocks, ROW_BLOCK)
    vocab_ids = jnp.arange(VOCAB_SIZE)

    def block_step(acc_pair, block_in):
        dw_acc, dg_acc = acc_pair
        h_rows, lab_rows, valid_rows = block_in
        h_f32 = h_rows.astype(jnp.float32)
        inv_rms = lax.rsqrt(jnp.mean(h_f32 * h_f32, axis=-1, keepdims=True) + NORM_EPS)
        x_hat = h_f32 * inv_rms
        x_norm = (x_hat * norm_gain).astype(jnp.bfloat16)
        logits = jnp.dot(x_norm, w_head, preferred_element_type=jnp.float32)
        row_max = jnp.max(logits, axis=-1, keepdims=True)
        exp_shift = jnp.exp(logits - row_max)
        sum_exp = jnp.sum(exp_shift, axis=-1, keepdims=True)
        log_norm = (row_max + jnp.log(sum_exp))[:, 0]
        onehot = (vocab_ids[None, :] == lab_rows[:, None]).astype(jnp.float32)
        target_logit = jnp.sum(onehot * logits, axis=-1)
        loss_rows = (log_norm - target_logit) * valid_rows
        d_logits = ((exp_shift / sum_exp - onehot) * (valid_rows / valid_count)[:, None]).astype(jnp.bfloat16)
        dx_norm = jnp.dot(d_logits, w_head.T, preferred_element_type=jnp.float32)
        dw_acc = dw_acc + jnp.dot(x_norm.T, d_logits, preferred_element_type=jnp.float32)
        dg_acc = dg_acc + jnp.sum(dx_norm * x_hat, axis=0)
        dx_hat = dx_norm * norm_gain
        d_rows = (inv_rms * (dx_hat - x_hat * jnp.mean(dx_hat * x_hat, axis=-1, keepdims=True))).astype(jnp.bfloat16)
        return (dw_acc, dg_acc), (loss_rows, d_rows)

    init_acc = (jnp.zeros((HIDDEN, VOCAB_SIZE), jnp.float32), jnp.zeros((HIDDEN,), jnp.float32))
    (d_head, d_gain), (loss_blocks, d_blocks) = lax.scan(block_step, init_acc, (rows_h, rows_lab, rows_valid))
    tok_loss = loss_blocks.reshape(BATCH_ALL, SEQ_LEN)
    loss_mean = jnp.sum(tok_loss) / valid_count
    d_hidden = d_blocks.reshape(BATCH_ALL, SEQ_LEN, HIDDEN)
    return tok_loss, loss_mean, d_hidden, d_gain, d_head
```

```python
import functools

import jax
import jax.numpy as jnp
import numpy as np
from jax import lax
from jax.experimental import pallas as pl
from jax.experimental.pallas import tpu as pltpu
from jax.sharding import PartitionSpec as P


NORM_EPS = 1e-5
BN = 512
N_CHUNK = 4
SHARED_SIZES = (3, 3)
COMMON_SIZES = (4, 4, 2, 2)
VMEM_LIMIT = 67043328


def logits_kernel(x_ref, w_ref, z_ref, m_ref, s_ref):
    @pl.when(pl.program_id(0) == 0)
    def _():
        m_ref[...] = jnp.full_like(m_ref, -jnp.inf)
        s_ref[...] = jnp.zeros_like(s_ref)

    sub = 512
    for j in range(w_ref.shape[1] // sub):
        z = jnp.dot(x_ref[...], w_ref[:, j * sub:(j + 1) * sub], preferred_element_type=jnp.float32)
        z_ref[:, j * sub:(j + 1) * sub] = z
        parts = [z[:, k * 128:(k + 1) * 128] for k in range(sub // 128)]
        m_old = m_ref[...]
        m_new = functools.reduce(jnp.maximum, parts, m_old)
        acc = s_ref[...] * jnp.exp(m_old - m_new)
        for part in parts:
            acc = acc + jnp.exp(part - m_new)
        s_ref[...] = acc
        m_ref[...] = m_new


def logits_pass(x_norm, w_head, block):
    rows, depth = x_norm.shape
    vocab = w_head.shape[1]
    return pl.pallas_call(
        logits_kernel,
        grid=(vocab // block,),
        in_specs=[pl.BlockSpec((rows, depth), lambda i: (0, 0)), pl.BlockSpec((depth, block), lambda i: (0, i))],
        out_specs=[pl.BlockSpec((rows, block), lambda i: (0, i)), pl.BlockSpec((rows, 128), lambda i: (0, 0)), pl.BlockSpec((rows, 128), lambda i: (0, 0))],
        out_shape=[jax.ShapeDtypeStruct((rows, vocab), jnp.float32), jax.ShapeDtypeStruct((rows, 128), jnp.float32), jax.ShapeDtypeStruct((rows, 128), jnp.float32)],
        compiler_params=pltpu.CompilerParams(vmem_limit_bytes=VMEM_LIMIT, dimension_semantics=('arbitrary',)),
        cost_estimate=pl.CostEstimate(flops=2 * rows * depth * vocab, bytes_accessed=vocab * (depth * 2 + rows * 4), transcendentals=rows * vocab),
        name='logits_pass',
    )(x_norm, w_head)


def dx_kernel(n_blocks, z_ref, w_ref, lse_ref, scale_ref, lab_ref, dx_ref, t_ref, dz_buf):
    i = pl.program_id(0)
    rows, block = z_ref.shape

    @pl.when(i == 0)
    def _():
        dx_ref[...] = jnp.zeros_like(dx_ref)
        t_ref[...] = jnp.zeros_like(t_ref)
        dz_buf[1] = jnp.zeros(dz_buf.shape[1:], dz_buf.dtype)

    now, before = lax.rem(i, 2), lax.rem(i + 1, 2)
    lse, scale, lab = lse_ref[...], scale_ref[...], lab_ref[...]
    lab = jnp.where(i < n_blocks, lab, -1)
    lane = lax.broadcasted_iota(jnp.int32, (rows, 128), 1)
    first = i * block
    n_sub = 4
    width = dx_ref.shape[1] // n_sub
    per_sub = block // 128 // n_sub
    hit_sum = t_ref[...]
    for j in range(n_sub):
        dz = dz_buf[before]
        dx_ref[:, j * width:(j + 1) * width] += lax.dot_general(dz, w_ref[j * width:(j + 1) * width, :], (((1,), (1,)), ((), ())), preferred_element_type=jnp.float32)
        for k in range(j * per_sub, (j + 1) * per_sub):
            z = z_ref[:, k * 128:(k + 1) * 128]
            hit = lab == lane + (first + k * 128)
            hit_sum = hit_sum + jnp.where(hit, z, 0.0)
            prob = jnp.exp(z - lse)
            dz_buf[now, :, k * 128:(k + 1) * 128] = (jnp.where(hit, prob - 1.0, prob) * scale).astype(jnp.bfloat16)
    t_ref[...] = hit_sum


def dx_pass(z, w_head, lse, scale, lab, block):
    rows, vocab = z.shape
    depth = w_head.shape[0]
    n_blocks = vocab // block
    row_spec = pl.BlockSpec((rows, 128), lambda i: (0, 0))
    return pl.pallas_call(
        functools.partial(dx_kernel, n_blocks),
        grid=(n_blocks + 1,),
        in_specs=[pl.BlockSpec((rows, block), lambda i: (0, jnp.minimum(i, n_blocks - 1))), pl.BlockSpec((depth, block), lambda i: (0, jnp.maximum(i - 1, 0))), row_spec, row_spec, row_spec],
        out_specs=[pl.BlockSpec((rows, depth), lambda i: (0, 0)), row_spec],
        out_shape=[jax.ShapeDtypeStruct((rows, depth), jnp.float32), jax.ShapeDtypeStruct((rows, 128), jnp.float32)],
        scratch_shapes=[pltpu.VMEM((2, rows, block), jnp.bfloat16)],
        compiler_params=pltpu.CompilerParams(vmem_limit_bytes=VMEM_LIMIT, dimension_semantics=('arbitrary',)),
        cost_estimate=pl.CostEstimate(flops=2 * rows * depth * vocab, bytes_accessed=vocab * (depth * 2 + rows * 4), transcendentals=rows * vocab),
        name='dx_pass',
    )(z, w_head, lse, scale, lab)


def prep_kernel(x_ref, g_ref, lse_ref, scale_ref, lab_ref, xn_ref, xt_ref, lse_out, scale_out, lab_out):
    xn = (x_ref[...] * g_ref[...]).astype(jnp.bfloat16)
    xn_ref[...] = xn
    xt_ref[...] = xn.T
    block = x_ref.shape[0]

    def wide(ref):
        return jnp.broadcast_to(ref[0], (128, block)).T

    lse_out[...] = wide(lse_ref)
    scale_out[...] = wide(scale_ref)
    lab_out[...] = wide(lab_ref).astype(jnp.int32)


def prep_pass(x_all, norm_gain, lse, scale, lab):
    tokens, depth = x_all.shape
    n, block = lse.shape
    row_spec = pl.BlockSpec((1, 1, block), lambda i: (i, 0, 0))
    wide_spec = pl.BlockSpec((block, 128), lambda i: (i, 0))
    return pl.pallas_call(
        prep_kernel,
        grid=(n,),
        in_specs=[pl.BlockSpec((block, depth), lambda i: (i, 0)), pl.BlockSpec((1, depth), lambda i: (0, 0)), row_spec, row_spec, row_spec],
        out_specs=[pl.BlockSpec((block, depth), lambda i: (i, 0)), pl.BlockSpec((depth, block), lambda i: (0, i)), wide_spec, wide_spec, wide_spec],
        out_shape=[jax.ShapeDtypeStruct((tokens, depth), jnp.bfloat16), jax.ShapeDtypeStruct((depth, tokens), jnp.bfloat16)] + [jax.ShapeDtypeStruct((tokens, 128), t) for t in (jnp.float32, jnp.float32, jnp.int32)],
        compiler_params=pltpu.CompilerParams(vmem_limit_bytes=VMEM_LIMIT, dimension_semantics=('arbitrary',)),
        cost_estimate=pl.CostEstimate(flops=8 * tokens * depth, bytes_accessed=8 * tokens * depth, transcendentals=0),
        name='prep_pass',
    )(x_all, norm_gain[None], lse[:, None], scale[:, None], lab[:, None])


def dw_kernel(n, halves, n_recv, lanes, has_prev, cols_ref, rcols_ref, w_ref, xn_hbm, xt_hbm, lse_hbm, scale_hbm, lab_hbm, *rest):
    recvs = rest[:n_recv]
    rest = rest[n_recv + (1 if has_prev else 0):]
    out_ref = rest[0]
    n_sends = 2 if halves else 1
    sends = rest[1:1 + n_sends]
    xn, xt, lse_v, scale_v, lab_v, dz_buf, o_buf, r_buf, in_sem, st_sem, out_sem, send_sem, rin_sem, rout_sem = rest[1 + n_sends:]
    i = pl.program_id(0)
    tokens, depth = xn.shape
    tok = tokens // N_CHUNK
    row = depth // N_CHUNK
    now, before = lax.rem(i, 2), lax.rem(i + 1, 2)

    def xn_copy(t):
        part = pl.ds(pl.multiple_of(t * tok, tok), tok)
        return pltpu.make_async_copy(xn_hbm.at[part, :], xn.at[part, :], in_sem.at[t])

    def xt_copy(t):
        part = pl.ds(pl.multiple_of(t * row, row), row)
        return pltpu.make_async_copy(xt_hbm.at[part, :], xt.at[part, :], in_sem.at[N_CHUNK + t])

    def stat_copies():
        return [pltpu.make_async_copy(src, dst, st_sem.at[k]) for k, (src, dst) in enumerate(((lse_hbm, lse_v), (scale_hbm, scale_v), (lab_hbm, lab_v)))]

    def tile(ref, r, block):
        return ref.at[pl.ds(pl.multiple_of(r * row, row), row), pl.ds(pl.multiple_of(block * BN, BN), BN)]

    def out_copy(step, t, slot):
        return pltpu.make_async_copy(o_buf.at[slot], tile(out_ref, t, cols_ref[step]), out_sem.at[slot])

    def send_copy(k, r, block, slot):
        return pltpu.make_async_copy(o_buf.at[slot], tile(sends[k], r, block), send_sem.at[slot])

    def finish_out(slot):
        out_copy(0, 0, slot).wait()
        send_copy(0, 0, 0, slot).wait()

    def rin_copy(lane, ref, r, block, slot):
        return pltpu.make_async_copy(tile(ref, r, block), r_buf.at[slot, lane], rin_sem.at[slot, lane])

    def rout_copy(lane, r, block, slot):
        return pltpu.make_async_copy(r_buf.at[slot, lane], tile(out_ref, r, block), rout_sem.at[slot, lane])

    def move_tiles(t):
        v = i * N_CHUNK + t
        slot, other = lax.rem(v, 2), lax.rem(v + 1, 2)
        for lane, entries in enumerate(lanes):
            total = sum(entry[4] for entry in entries)
            at = 0
            for k, first_col, first_row, u0, count, per_block in entries:
                @pl.when((v >= at + 1) & (v < at + 1 + count))
                def _(at=at, first_col=first_col, first_row=first_row, u0=u0, per_block=per_block):
                    u = v - 1 - at + u0
                    rin_copy(lane, recvs[0], 0, 0, other).wait()
                    rout_copy(lane, first_row + lax.rem(u, per_block), rcols_ref[first_col + u // per_block], other).start()

                at += count

            @pl.when((v >= 2) & (v < total + 2))
            def _():
                rout_copy(lane, 0, 0, slot).wait()

            at = 0
            for k, first_col, first_row, u0, count, per_block in entries:
                @pl.when((v >= at) & (v < at + count))
                def _(at=at, k=k, u0=u0, per_block=per_block):
                    u = v - at + u0
                    rin_copy(lane, recvs[k], lax.rem(u, per_block), u // per_block, slot).start()

                at += count

    def make_dz(t):
        part = pl.ds(pl.multiple_of(t * tok, tok), tok)
        z = jnp.dot(xn[part, :], w_ref[...], preferred_element_type=jnp.float32)
        lse, scale, lab = lse_v[part, :], scale_v[part, :], lab_v[part, :]
        lane_id = lax.broadcasted_iota(jnp.int32, (tok, 128), 1)
        first = cols_ref[jnp.minimum(i, n - 1)] * BN
        for k in range(BN // 128):
            prob = jnp.exp(z[:, k * 128:(k + 1) * 128] - lse)
            hit = lab == lane_id + (first + k * 128)
            dz_buf[now, part, k * 128:(k + 1) * 128] = (jnp.where(hit, prob - 1.0, prob) * scale).astype(jnp.bfloat16)

    def make_dw(t):
        part = pl.ds(pl.multiple_of(t * row, row), row)
        o_buf[lax.rem(t, 2)] = jnp.dot(xt[part, :], dz_buf[before], preferred_element_type=jnp.float32)

    def flush(t):
        slot = lax.rem(t, 2)
        out_copy(i - 1, t, slot).start()
        if halves:
            @pl.when(t < N_CHUNK // 2)
            def _():
                send_copy(0, t, i - 1, slot).start()

            @pl.when(t >= N_CHUNK // 2)
            def _():
                send_copy(1, t - N_CHUNK // 2, i - 1, slot).start()
        else:
            send_copy(0, t, i - 1, slot).start()

    def loop(do_dz, do_dw):
        def body(t, carry):
            move_tiles(t)
            if do_dw:
                @pl.when((i > 1) | (t > 1))
                def _():
                    finish_out(lax.rem(t, 2))

                @pl.when(i == 1)
                def _():
                    xt_copy(t).wait()
            else:
                xn_copy(t).wait()

                @pl.when(t + 2 < N_CHUNK)
                def _():
                    xn_copy(t + 2).start()

                xt_copy(t).start()
            if do_dz:
                make_dz(t)
            if do_dw:
                make_dw(t)
                flush(t)
            return carry

        lax.fori_loop(0, N_CHUNK, body, 0)

    @pl.when(i == 0)
    def _():
        xn_copy(0).start()
        for copy in stat_copies():
            copy.start()
        xn_copy(1).start()
        for copy in stat_copies():
            copy.wait()
        loop(True, False)

    @pl.when((i > 0) & (i < n))
    def _():
        loop(True, True)

    @pl.when(i == n)
    def _():
        loop(False, True)
        finish_out(0)
        finish_out(1)


def plan_lanes(recvs, row, n):
    room = (n + 1) * N_CHUNK - 2
    lanes, left, first_col = [], 0, 0
    for k, (array, first_row) in enumerate(recvs):
        per_block = array.shape[0] // row
        total = per_block * (array.shape[1] // BN)
        done = 0
        while done < total:
            if left == 0:
                lanes.append([])
                left = room
            take = min(left, total - done)
            lanes[-1].append((k, first_col, first_row, done, take, per_block))
            done += take
            left -= take
        first_col += array.shape[1] // BN
    return tuple(tuple(lane) for lane in lanes)


def dw_pass(cols, halves, recvs, rcols, prev, w_head, xn, xt, lse, scale, lab):
    n = cols.shape[0]
    depth, vocab = w_head.shape
    tokens = xn.shape[0]
    row = depth // N_CHUNK
    hbm = pl.BlockSpec(memory_space=pl.ANY)
    operands = [w_head, xn, xt, lse, scale, lab, *[r for r, _ in recvs]]
    if prev is not None:
        operands.append(prev)
    lanes = plan_lanes(recvs, row, n)
    n_lanes = max(len(lanes), 1)
    send_rows = [depth // 2] * 2 if halves else [depth]
    out_shape = [jax.ShapeDtypeStruct((depth, vocab), jnp.float32)] + [jax.ShapeDtypeStruct((r, n * BN), jnp.float32) for r in send_rows]
    grid_spec = pltpu.PrefetchScalarGridSpec(
        num_scalar_prefetch=2,
        grid=(n + 1,),
        in_specs=[pl.BlockSpec((depth, BN), lambda i, cols, rcols: (0, cols[jnp.minimum(i, n - 1)]))] + [hbm] * (len(operands) - 1),
        out_specs=[hbm] * len(out_shape),
        scratch_shapes=[
            pltpu.VMEM((tokens, depth), jnp.bfloat16),
            pltpu.VMEM((depth, tokens), jnp.bfloat16),
            pltpu.VMEM((tokens, 128), jnp.float32),
            pltpu.VMEM((tokens, 128), jnp.float32),
            pltpu.VMEM((tokens, 128), jnp.int32),
            pltpu.VMEM((2, tokens, BN), jnp.bfloat16),
            pltpu.VMEM((2, row, BN), jnp.float32),
            pltpu.VMEM((2, n_lanes, row, BN) if lanes else (2, 1, 8, 128), jnp.float32),
            pltpu.SemaphoreType.DMA((2 * N_CHUNK,)),
            pltpu.SemaphoreType.DMA((3,)),
            pltpu.SemaphoreType.DMA((2,)),
            pltpu.SemaphoreType.DMA((2,)),
            pltpu.SemaphoreType.DMA((2, n_lanes)),
            pltpu.SemaphoreType.DMA((2, n_lanes)),
        ],
    )
    width = n * BN
    return pl.pallas_call(
        functools.partial(dw_kernel, n, halves, len(recvs), lanes, prev is not None),
        grid_spec=grid_spec,
        out_shape=out_shape,
        input_output_aliases={} if prev is None else {2 + len(operands) - 1: 0},
        compiler_params=pltpu.CompilerParams(vmem_limit_bytes=VMEM_LIMIT, dimension_semantics=('arbitrary',)),
        cost_estimate=pl.CostEstimate(flops=4 * tokens * depth * width, bytes_accessed=depth * width * 10, transcendentals=tokens * width),
    )(cols, rcols, *operands)


def place_kernel(n_recv, starts, at_row, at_col, *refs):
    recvs, out_ref = refs[:n_recv], refs[n_recv + 1]
    i = pl.program_id(0)
    for k, ref in enumerate(recvs):
        @pl.when((i >= starts[k]) & (i < starts[k + 1]))
        def _(ref=ref):
            out_ref[...] = ref[...]


def place_pass(recvs, rcols, prev):
    depth = prev.shape[0]
    half = depth // 2
    steps, sizes, first_col = [], [], 0
    for array, first_row in recvs:
        per_block = array.shape[0] // half
        for block in range(array.shape[1] // BN):
            for r in range(per_block):
                steps.append((first_row // (N_CHUNK // 2) + r, first_col + block))
        first_col += array.shape[1] // BN
        sizes.append((per_block, per_block * (array.shape[1] // BN)))
    starts = [0] + [int(v) for v in np.cumsum([size for _, size in sizes])]
    at_row = jnp.asarray([r for r, _ in steps], jnp.int32)
    at_col = rcols[np.asarray([c for _, c in steps])]

    def recv_spec(k):
        per_block, size = sizes[k]

        def at(i, at_row, at_col):
            u = jnp.clip(i - starts[k], 0, size - 1)
            return lax.rem(u, per_block), lax.div(u, per_block)

        return pl.BlockSpec((half, BN), at)

    return pl.pallas_call(
        functools.partial(place_kernel, len(recvs), tuple(starts)),
        grid_spec=pltpu.PrefetchScalarGridSpec(
            num_scalar_prefetch=2,
            grid=(starts[-1],),
            in_specs=[recv_spec(k) for k in range(len(recvs))] + [pl.BlockSpec(memory_space=pl.ANY)],
            out_specs=pl.BlockSpec((half, BN), lambda i, at_row, at_col: (at_row[i], at_col[i])),
        ),
        out_shape=jax.ShapeDtypeStruct(prev.shape, prev.dtype),
        input_output_aliases={2 + len(recvs): 0},
        compiler_params=pltpu.CompilerParams(vmem_limit_bytes=VMEM_LIMIT, dimension_semantics=('arbitrary',)),
        cost_estimate=pl.CostEstimate(flops=half * BN * starts[-1], bytes_accessed=8 * half * BN * starts[-1], transcendentals=0),
        name='place_pass',
    )(at_row, at_col, *[r for r, _ in recvs], prev)


def solution(mesh):
    tp_size, cp_size, dp_size = mesh.shape['tp'], mesh.shape['cp'], mesh.shape['dp']
    from_next_pairs = [(cp_idx + 1, cp_idx) for cp_idx in range(cp_size - 1)]
    from_prev_pairs = [(cp_idx - 1, cp_idx) for cp_idx in range(1, cp_size)]
    tp_swap = [(t, 1 - t) for t in range(tp_size)]
    cp_swap = [(c, 1 - c) for c in range(cp_size)]
    core_swap = [(d, d ^ 1) for d in range(dp_size)]
    x_swap = [(d, d ^ 2) for d in range(dp_size)]

    def local_fn(hidden, tokens, seq_lens, norm_gain, w_head):
        n_seqs, local_len, depth = hidden.shape
        rows = n_seqs * local_len
        seg_len = local_len // 2
        vocab_local = w_head.shape[1]
        cp_rank = lax.axis_index('cp')
        tp_rank = lax.axis_index('tp')
        dp_rank = lax.axis_index('dp')
        core = dp_rank % 2

        def swap(v, axis, pairs):
            return lax.ppermute(v, axis, pairs)

        h_f32 = hidden.reshape(rows, depth).astype(jnp.float32)
        inv_rms = lax.rsqrt(jnp.mean(h_f32 * h_f32, axis=-1, keepdims=True) + NORM_EPS)
        x_hat = h_f32 * inv_rms
        x_norm = (x_hat * norm_gain).astype(jnp.bfloat16)
        x_all = lax.all_gather(x_hat, ('cp', 'dp'), tiled=True)

        next_first = lax.ppermute(tokens[:, 0], 'cp', from_next_pairs)
        prev_second = lax.ppermute(tokens[:, seg_len], 'cp', from_prev_pairs)
        first_end = jnp.where(cp_rank == cp_size - 1, tokens[:, seg_len], next_first)
        labels = jnp.concatenate([tokens[:, 1:seg_len], first_end[:, None], tokens[:, seg_len + 1:], prev_second[:, None]], axis=1)
        seg_pos = jnp.arange(seg_len)
        positions = jnp.concatenate([cp_rank * seg_len + seg_pos, (2 * cp_size - 1 - cp_rank) * seg_len + seg_pos])
        valid_mask = (positions[None, :] + 1 < seq_lens[:, None]).astype(jnp.float32)

        z, m_lane, s_lane = logits_pass(x_norm, w_head, 1024)
        m_loc = jnp.max(m_lane, axis=-1)
        s_loc = jnp.sum(s_lane * jnp.exp(m_lane - m_loc[:, None]), axis=-1)

        stats = jnp.stack([m_loc, s_loc, labels.reshape(rows).astype(jnp.float32), valid_mask.reshape(rows)])
        stats = lax.all_gather(stats, ('tp', 'cp', 'dp')).reshape(tp_size, cp_size * dp_size, 4, rows)
        glob_max = jnp.max(stats[:, :, 0], axis=0)
        log_norm_all = glob_max + jnp.log(jnp.sum(stats[:, :, 1] * jnp.exp(stats[:, :, 0] - glob_max), axis=0))
        valid_all = stats[0, :, 3]
        valid_count = jnp.sum(valid_all)
        scale_all = valid_all / valid_count
        lab_f32 = stats[0, :, 2] - (tp_rank * vocab_local).astype(jnp.float32)

        def wide(v):
            return jnp.broadcast_to(v.reshape(-1, 1), (v.size, 128))

        mine = cp_rank * dp_size + dp_rank

        def own(v):
            return lax.dynamic_index_in_dim(v, mine, axis=0, keepdims=False)

        log_norm = own(log_norm_all)
        dx_part, t_lane = dx_pass(z, w_head, wide(log_norm), wide(own(scale_all)), wide(own(lab_f32).astype(jnp.int32)), 1024)
        t_part = jnp.sum(t_lane, axis=-1)
        dx_part, x_all = lax.optimization_barrier((dx_part, x_all))
        xn_all, xt_all, lse_w, scale_w, lab_w = prep_pass(x_all, norm_gain, log_norm_all, scale_all, lab_f32)
        dx_norm = dx_part + swap(dx_part, 'tp', tp_swap)
        target_logit = t_part + swap(t_part, 'tp', tp_swap)
        tok_loss = (log_norm - target_logit).reshape(n_seqs, local_len) * valid_mask

        sums = jnp.concatenate([jnp.sum(dx_norm * x_hat, axis=0), jnp.full((128,), jnp.sum(tok_loss))])
        sums = sums + swap(sums, 'dp', core_swap)
        sums = sums + swap(sums, 'dp', x_swap)
        sums = sums + swap(sums, 'cp', cp_swap)
        d_gain = sums[:depth]
        loss_mean = sums[depth] / valid_count
        dx_hat = dx_norm * norm_gain
        d_hidden = (inv_rms * (dx_hat - x_hat * jnp.mean(dx_hat * x_hat, axis=-1, keepdims=True))).astype(jnp.bfloat16)

        n_blocks = vocab_local // BN
        shared, common = SHARED_SIZES, COMMON_SIZES
        n_shared, n_common = sum(shared), sum(common)
        assert 4 * n_shared + 2 * n_common == n_blocks
        role = (dp_rank // 2 + cp_rank) % 2

        def shared_cols(k, who, part):
            first = sum(shared[:k])
            return (who * 2 * n_shared + part * n_shared + first + jnp.arange(shared[k])).astype(jnp.int32)

        def common_cols(k, part):
            first = sum(common[:k])
            return (4 * n_shared + part * n_common + first + jnp.arange(common[k])).astype(jnp.int32)

        lower = N_CHUNK // 2
        out = None

        def run(cols, halves, arrived):
            recvs = [pair for pair, _ in arrived]
            rcols = jnp.concatenate([c for _, c in arrived]) if arrived else jnp.zeros((1,), jnp.int32)
            return dw_pass(cols, halves, recvs, rcols, out, w_head, xn_all, xt_all, lse_w, scale_w, lab_w)

        from_core, from_chip, passed_on, from_core_common = {}, {}, {}, {}

        def share(k, send_x, send_y):
            cols = shared_cols(k, role, 1 - core)
            from_core[k] = [((swap(send_x, 'dp', core_swap), 0), cols), ((swap(send_y, 'dp', core_swap), lower), cols)]
            cols = shared_cols(k, 1 - role, core)
            from_chip[k] = [((swap(send_x, 'dp', x_swap), 0), cols), ((swap(send_y, 'cp', cp_swap), lower), cols)]

        def pass_on(k):
            nonlocal out
            cols = shared_cols(k, 1 - role, 1 - core)
            (up, _), (low, _) = [pair for pair, _ in from_chip[k]]
            up, low, out = lax.optimization_barrier((up, low, out))
            from_chip[k] = [((up, 0), from_chip[k][0][1]), ((low, lower), from_chip[k][1][1])]
            passed_on[k] = [((swap(up, 'dp', core_swap), 0), cols), ((swap(low, 'dp', core_swap), lower), cols)]

        def share_common(k, send):
            from_core_common[k] = [((swap(send, 'dp', core_swap), 0), common_cols(k, 1 - core))]

        out, *sent = run(shared_cols(0, role, core), True, [])
        share(0, *sent)
        out, *sent = run(shared_cols(1, role, core), True, [])
        share(1, *sent)
        out, *sent = run(common_cols(0, core), False, from_core[0])
        share_common(0, *sent)
        pass_on(0)
        out, *sent = run(common_cols(1, core), False, from_core[1] + from_chip[0])
        share_common(1, *sent)
        out, *sent = run(common_cols(2, core), False, passed_on[0] + from_core_common[0])
        share_common(2, *sent)
        pass_on(1)
        out, *sent = run(common_cols(3, core), False, from_chip[1] + from_core_common[1])
        share_common(3, *sent)
        last = passed_on[1] + from_core_common[2] + from_core_common[3]
        d_head = place_pass([pair for pair, _ in last], jnp.concatenate([c for _, c in last]), out)
        return tok_loss, loss_mean, d_hidden.reshape(hidden.shape), d_gain, d_head

    return jax.shard_map(local_fn, mesh=mesh, in_specs=(P('dp', 'cp', None), P('dp', 'cp'), P('dp'), P(None), P(None, 'tp')), out_specs=(P('dp', 'cp'), P(), P('dp', 'cp', None), P(None), P(None, 'tp')), check_vma=False)
```

```python
import functools

import jax
import jax.numpy as jnp
import numpy as np
from jax import lax
from jax.experimental import pallas as pl
from jax.experimental.pallas import tpu as pltpu
from jax.sharding import PartitionSpec as P


NORM_EPS = 1e-5
BN = 512
N_CHUNK = 4
SHARED_SIZES = (2, 4)
COMMON_SIZES = (5, 4, 3)
VMEM_LIMIT = 67043328


def logits_kernel(x_ref, w_ref, z_ref, m_ref, s_ref):
    @pl.when(pl.program_id(0) == 0)
    def _():
        m_ref[...] = jnp.full_like(m_ref, -jnp.inf)
        s_ref[...] = jnp.zeros_like(s_ref)

    sub = 512
    for j in range(w_ref.shape[1] // sub):
        z = jnp.dot(x_ref[...], w_ref[:, j * sub:(j + 1) * sub], preferred_element_type=jnp.float32)
        z_ref[:, j * sub:(j + 1) * sub] = z
        parts = [z[:, k * 128:(k + 1) * 128] for k in range(sub // 128)]
        m_old = m_ref[...]
        m_new = functools.reduce(jnp.maximum, parts, m_old)
        acc = s_ref[...] * jnp.exp(m_old - m_new)
        for part in parts:
            acc = acc + jnp.exp(part - m_new)
        s_ref[...] = acc
        m_ref[...] = m_new


def logits_pass(x_norm, w_head, block):
    rows, depth = x_norm.shape
    vocab = w_head.shape[1]
    return pl.pallas_call(
        logits_kernel,
        grid=(vocab // block,),
        in_specs=[pl.BlockSpec((rows, depth), lambda i: (0, 0)), pl.BlockSpec((depth, block), lambda i: (0, i))],
        out_specs=[pl.BlockSpec((rows, block), lambda i: (0, i)), pl.BlockSpec((rows, 128), lambda i: (0, 0)), pl.BlockSpec((rows, 128), lambda i: (0, 0))],
        out_shape=[jax.ShapeDtypeStruct((rows, vocab), jnp.float32), jax.ShapeDtypeStruct((rows, 128), jnp.float32), jax.ShapeDtypeStruct((rows, 128), jnp.float32)],
        compiler_params=pltpu.CompilerParams(vmem_limit_bytes=VMEM_LIMIT, dimension_semantics=('arbitrary',)),
        cost_estimate=pl.CostEstimate(flops=2 * rows * depth * vocab, bytes_accessed=vocab * (depth * 2 + rows * 4), transcendentals=rows * vocab),
        name='logits_pass',
    )(x_norm, w_head)


def dx_kernel(n_blocks, z_ref, w_ref, lse_ref, scale_ref, lab_ref, dx_ref, t_ref, dz_buf):
    i = pl.program_id(0)
    rows, block = z_ref.shape

    @pl.when(i == 0)
    def _():
        dx_ref[...] = jnp.zeros_like(dx_ref)
        t_ref[...] = jnp.zeros_like(t_ref)
        dz_buf[1] = jnp.zeros(dz_buf.shape[1:], dz_buf.dtype)

    now, before = lax.rem(i, 2), lax.rem(i + 1, 2)
    lse, scale, lab = lse_ref[...], scale_ref[...], lab_ref[...]
    lab = jnp.where(i < n_blocks, lab, -1)
    lane = lax.broadcasted_iota(jnp.int32, (rows, 128), 1)
    first = i * block
    n_sub = 4
    width = dx_ref.shape[1] // n_sub
    per_sub = block // 128 // n_sub
    hit_sum = t_ref[...]
    for j in range(n_sub):
        dz = dz_buf[before]
        dx_ref[:, j * width:(j + 1) * width] += lax.dot_general(dz, w_ref[j * width:(j + 1) * width, :], (((1,), (1,)), ((), ())), preferred_element_type=jnp.float32)
        for k in range(j * per_sub, (j + 1) * per_sub):
            z = z_ref[:, k * 128:(k + 1) * 128]
            hit = lab == lane + (first + k * 128)
            hit_sum = hit_sum + jnp.where(hit, z, 0.0)
            prob = jnp.exp(z - lse)
            dz_buf[now, :, k * 128:(k + 1) * 128] = (jnp.where(hit, prob - 1.0, prob) * scale).astype(jnp.bfloat16)
    t_ref[...] = hit_sum


def dx_pass(z, w_head, lse, scale, lab, block):
    rows, vocab = z.shape
    depth = w_head.shape[0]
    n_blocks = vocab // block
    row_spec = pl.BlockSpec((rows, 128), lambda i: (0, 0))
    return pl.pallas_call(
        functools.partial(dx_kernel, n_blocks),
        grid=(n_blocks + 1,),
        in_specs=[pl.BlockSpec((rows, block), lambda i: (0, jnp.minimum(i, n_blocks - 1))), pl.BlockSpec((depth, block), lambda i: (0, jnp.maximum(i - 1, 0))), row_spec, row_spec, row_spec],
        out_specs=[pl.BlockSpec((rows, depth), lambda i: (0, 0)), row_spec],
        out_shape=[jax.ShapeDtypeStruct((rows, depth), jnp.float32), jax.ShapeDtypeStruct((rows, 128), jnp.float32)],
        scratch_shapes=[pltpu.VMEM((2, rows, block), jnp.bfloat16)],
        compiler_params=pltpu.CompilerParams(vmem_limit_bytes=VMEM_LIMIT, dimension_semantics=('arbitrary',)),
        cost_estimate=pl.CostEstimate(flops=2 * rows * depth * vocab, bytes_accessed=vocab * (depth * 2 + rows * 4), transcendentals=rows * vocab),
        name='dx_pass',
    )(z, w_head, lse, scale, lab)


def prep_kernel(mine_ref, x_ref, g_ref, *refs):
    xn_ref, xt_ref, lse_out, scale_out, lab_out = refs[-5:]
    source = jnp.bitwise_xor(mine_ref[0], pl.program_id(0))
    stats = refs[0][...]
    for k in range(1, len(refs) - 5):
        stats = jnp.where(source == k, refs[k][...], stats)
    xn = (x_ref[...] * g_ref[...]).astype(jnp.bfloat16)
    xn_ref[...] = xn
    xt_ref[...] = xn.T
    block = x_ref.shape[0]

    def wide(k):
        return jnp.broadcast_to(stats[k:k + 1, :], (128, block)).T

    lse_out[...] = wide(0)
    scale_out[...] = wide(2)
    lab_out[...] = wide(1).astype(jnp.int32)


def prep_pass(mine, x_all, norm_gain, stats):
    tokens, depth = x_all.shape
    n = len(stats)
    n_stats, block = stats[0].shape
    wide_spec = pl.BlockSpec((block, 128), lambda i, mine: (i, 0))
    return pl.pallas_call(
        prep_kernel,
        grid_spec=pltpu.PrefetchScalarGridSpec(
            num_scalar_prefetch=1,
            grid=(n,),
            in_specs=[pl.BlockSpec((block, depth), lambda i, mine: (i, 0)), pl.BlockSpec((1, depth), lambda i, mine: (0, 0)), *[pl.BlockSpec((n_stats, block), lambda i, mine: (0, 0))] * n],
            out_specs=[pl.BlockSpec((block, depth), lambda i, mine: (i, 0)), pl.BlockSpec((depth, block), lambda i, mine: (0, i)), wide_spec, wide_spec, wide_spec],
        ),
        out_shape=[jax.ShapeDtypeStruct((tokens, depth), jnp.bfloat16), jax.ShapeDtypeStruct((depth, tokens), jnp.bfloat16)] + [jax.ShapeDtypeStruct((tokens, 128), t) for t in (jnp.float32, jnp.float32, jnp.int32)],
        compiler_params=pltpu.CompilerParams(vmem_limit_bytes=VMEM_LIMIT, dimension_semantics=('arbitrary',)),
        cost_estimate=pl.CostEstimate(flops=8 * tokens * depth, bytes_accessed=8 * tokens * depth, transcendentals=0),
        name='prep_pass',
    )(mine, x_all, norm_gain[None], *stats)


def dw_kernel(n, entry, halves, n_recv, lanes, has_prev, bases_ref, w_ref, xn_hbm, xt_hbm, lse_hbm, scale_hbm, lab_hbm, *rest):
    recvs = rest[:n_recv]
    rest = rest[n_recv + (1 if has_prev else 0):]
    out_ref = rest[0]
    n_sends = 2 if halves else 1
    sends = rest[1:1 + n_sends]
    xn, xt, lse_v, scale_v, lab_v, dz_buf, o_buf, r_buf, in_sem, st_sem, out_sem, send_sem, rin_sem, rout_sem = rest[1 + n_sends:]
    i = pl.program_id(0)
    tokens, depth = xn.shape
    tok = tokens // N_CHUNK
    row = depth // N_CHUNK
    now, before = lax.rem(i, 2), lax.rem(i + 1, 2)

    def xn_copy(t):
        part = pl.ds(pl.multiple_of(t * tok, tok), tok)
        return pltpu.make_async_copy(xn_hbm.at[part, :], xn.at[part, :], in_sem.at[t])

    def xt_copy(t):
        part = pl.ds(pl.multiple_of(t * row, row), row)
        return pltpu.make_async_copy(xt_hbm.at[part, :], xt.at[part, :], in_sem.at[N_CHUNK + t])

    def stat_copies(t):
        part = pl.ds(pl.multiple_of(t * tok, tok), tok)
        return [pltpu.make_async_copy(src.at[part, :], dst.at[part, :], st_sem.at[k, t]) for k, (src, dst) in enumerate(((lse_hbm, lse_v), (scale_hbm, scale_v), (lab_hbm, lab_v)))]

    def tile(ref, r, block):
        return ref.at[pl.ds(pl.multiple_of(r * row, row), row), pl.ds(pl.multiple_of(block * BN, BN), BN)]

    def out_copy(step, t, slot):
        return pltpu.make_async_copy(o_buf.at[slot], tile(out_ref, t, bases_ref[entry] + step), out_sem.at[slot])

    def send_copy(k, r, block, slot):
        return pltpu.make_async_copy(o_buf.at[slot], tile(sends[k], r, block), send_sem.at[slot])

    def finish_out(slot):
        out_copy(0, 0, slot).wait()
        send_copy(0, 0, 0, slot).wait()

    def rin_copy(lane, ref, r, block, slot):
        return pltpu.make_async_copy(tile(ref, r, block), r_buf.at[slot, lane], rin_sem.at[slot, lane])

    def rout_copy(lane, r, block, slot):
        return pltpu.make_async_copy(r_buf.at[slot, lane], tile(out_ref, r, block), rout_sem.at[slot, lane])

    def move_tiles(t):
        v = i * N_CHUNK + t
        slot, other = lax.rem(v, 2), lax.rem(v + 1, 2)
        for lane, entries in enumerate(lanes):
            total = sum(entry[4] for entry in entries)
            at = 0
            for k, where, first_row, u0, count, per_block in entries:
                @pl.when((v >= at + 1) & (v < at + 1 + count))
                def _(at=at, where=where, first_row=first_row, u0=u0, per_block=per_block):
                    u = v - 1 - at + u0
                    rin_copy(lane, recvs[0], 0, 0, other).wait()
                    rout_copy(lane, first_row + lax.rem(u, per_block), bases_ref[where] + u // per_block, other).start()

                at += count

            @pl.when((v >= 2) & (v < total + 2))
            def _():
                rout_copy(lane, 0, 0, slot).wait()

            at = 0
            for k, where, first_row, u0, count, per_block in entries:
                @pl.when((v >= at) & (v < at + count))
                def _(at=at, k=k, u0=u0, per_block=per_block):
                    u = v - at + u0
                    rin_copy(lane, recvs[k], lax.rem(u, per_block), u // per_block, slot).start()

                at += count

    def make_dz(t):
        part = pl.ds(pl.multiple_of(t * tok, tok), tok)
        z = jnp.dot(xn[part, :], w_ref[...], preferred_element_type=jnp.float32)
        lse, scale, lab = lse_v[part, :], scale_v[part, :], lab_v[part, :]
        lane_id = lax.broadcasted_iota(jnp.int32, (tok, 128), 1)
        first = (bases_ref[entry] + jnp.minimum(i, n - 1)) * BN
        for k in range(BN // 128):
            prob = jnp.exp(z[:, k * 128:(k + 1) * 128] - lse)
            hit = lab == lane_id + (first + k * 128)
            dz_buf[now, part, k * 128:(k + 1) * 128] = (jnp.where(hit, prob - 1.0, prob) * scale).astype(jnp.bfloat16)

    def make_dw(t):
        part = pl.ds(pl.multiple_of(t * row, row), row)
        o_buf[lax.rem(t, 2)] = jnp.dot(xt[part, :], dz_buf[before], preferred_element_type=jnp.float32)

    def flush(t):
        slot = lax.rem(t, 2)
        out_copy(i - 1, t, slot).start()
        if halves:
            @pl.when(t < N_CHUNK // 2)
            def _():
                send_copy(0, t, i - 1, slot).start()

            @pl.when(t >= N_CHUNK // 2)
            def _():
                send_copy(1, t - N_CHUNK // 2, i - 1, slot).start()
        else:
            send_copy(0, t, i - 1, slot).start()

    def loop(do_dz, do_dw):
        def body(t, carry):
            move_tiles(t)
            if do_dw:
                @pl.when((i > 1) | (t > 1))
                def _():
                    finish_out(lax.rem(t, 2))

                @pl.when(i == 1)
                def _():
                    xt_copy(t).wait()
            else:
                xn_copy(t).wait()
                for copy in stat_copies(t):
                    copy.wait()

                @pl.when(t + 2 < N_CHUNK)
                def _():
                    xn_copy(t + 2).start()
                    for copy in stat_copies(t + 2):
                        copy.start()

                xt_copy(t).start()
            if do_dz:
                make_dz(t)
            if do_dw:
                make_dw(t)
                flush(t)
            return carry

        lax.fori_loop(0, N_CHUNK, body, 0)

    @pl.when(i == 0)
    def _():
        for t in range(2):
            xn_copy(t).start()
            for copy in stat_copies(t):
                copy.start()
        loop(True, False)

    @pl.when((i > 0) & (i < n))
    def _():
        loop(True, True)

    @pl.when(i == n)
    def _():
        loop(False, True)
        finish_out(0)
        finish_out(1)


def plan_lanes(recvs, row, n):
    room = (n + 1) * N_CHUNK - 2
    lanes, left = [], 0
    for k, (array, first_row, where) in enumerate(recvs):
        per_block = array.shape[0] // row
        total = per_block * (array.shape[1] // BN)
        done = 0
        while done < total:
            if left == 0:
                lanes.append([])
                left = room
            take = min(left, total - done)
            lanes[-1].append((k, where, first_row, done, take, per_block))
            done += take
            left -= take
    return tuple(tuple(lane) for lane in lanes)


def dw_pass(n, entry, bases, halves, recvs, prev, w_head, xn, xt, lse, scale, lab):
    depth, vocab = w_head.shape
    tokens = xn.shape[0]
    row = depth // N_CHUNK
    hbm = pl.BlockSpec(memory_space=pl.ANY)
    operands = [w_head, xn, xt, lse, scale, lab, *[r for r, _, _ in recvs]]
    if prev is not None:
        operands.append(prev)
    lanes = plan_lanes(recvs, row, n)
    n_lanes = max(len(lanes), 1)
    send_rows = [depth // 2] * 2 if halves else [depth]
    out_shape = [jax.ShapeDtypeStruct((depth, vocab), jnp.float32)] + [jax.ShapeDtypeStruct((r, n * BN), jnp.float32) for r in send_rows]
    grid_spec = pltpu.PrefetchScalarGridSpec(
        num_scalar_prefetch=1,
        grid=(n + 1,),
        in_specs=[pl.BlockSpec((depth, BN), lambda i, bases: (0, bases[entry] + jnp.minimum(i, n - 1)))] + [hbm] * (len(operands) - 1),
        out_specs=[hbm] * len(out_shape),
        scratch_shapes=[
            pltpu.VMEM((tokens, depth), jnp.bfloat16),
            pltpu.VMEM((depth, tokens), jnp.bfloat16),
            pltpu.VMEM((tokens, 128), jnp.float32),
            pltpu.VMEM((tokens, 128), jnp.float32),
            pltpu.VMEM((tokens, 128), jnp.int32),
            pltpu.VMEM((2, tokens, BN), jnp.bfloat16),
            pltpu.VMEM((2, row, BN), jnp.float32),
            pltpu.VMEM((2, n_lanes, row, BN) if lanes else (2, 1, 8, 128), jnp.float32),
            pltpu.SemaphoreType.DMA((2 * N_CHUNK,)),
            pltpu.SemaphoreType.DMA((3, N_CHUNK)),
            pltpu.SemaphoreType.DMA((2,)),
            pltpu.SemaphoreType.DMA((2,)),
            pltpu.SemaphoreType.DMA((2, n_lanes)),
            pltpu.SemaphoreType.DMA((2, n_lanes)),
        ],
    )
    width = n * BN
    return pl.pallas_call(
        functools.partial(dw_kernel, n, entry, halves, len(recvs), lanes, prev is not None),
        grid_spec=grid_spec,
        out_shape=out_shape,
        input_output_aliases={} if prev is None else {1 + len(operands) - 1: 0},
        compiler_params=pltpu.CompilerParams(vmem_limit_bytes=VMEM_LIMIT, dimension_semantics=('arbitrary',)),
        cost_estimate=pl.CostEstimate(flops=4 * tokens * depth * width, bytes_accessed=depth * width * 10, transcendentals=tokens * width),
    )(bases, *operands)


def place_kernel(tiles, n_recv, bases_ref, *rest):
    recvs = rest[:n_recv]
    out_ref, buf, in_sem, out_sem = rest[n_recv + 1:]
    slots = buf.shape[0]

    def tile(ref, r, block):
        half = buf.shape[1]
        return ref.at[pl.ds(r * half, half), pl.ds(pl.multiple_of(block * BN, BN), BN)]

    def load(u):
        k, r, block, _, _ = tiles[u]
        return pltpu.make_async_copy(tile(recvs[k], r, block), buf.at[u % slots], in_sem.at[u % slots])

    def store(u):
        _, _, block, to_row, where = tiles[u]
        return pltpu.make_async_copy(buf.at[u % slots], tile(out_ref, to_row, bases_ref[where] + block), out_sem.at[u % slots])

    ahead = slots // 2
    n = len(tiles)
    for u in range(min(ahead, n)):
        load(u).start()
    for u in range(n):
        load(u).wait()
        store(u).start()
        if u + ahead < n:
            if u + ahead >= slots:
                store(u + ahead - slots).wait()
            load(u + ahead).start()
    for u in range(max(n - slots, 0), n):
        store(u).wait()


def place_pass(recvs, bases, prev):
    depth = prev.shape[0]
    half = depth // 2
    tiles = []
    for k, (array, first_row, where) in enumerate(recvs):
        for block in range(array.shape[1] // BN):
            for r in range(array.shape[0] // half):
                tiles.append((k, r, block, first_row // (N_CHUNK // 2) + r, where))
    hbm = pl.BlockSpec(memory_space=pl.ANY)
    slots = 12
    return pl.pallas_call(
        functools.partial(place_kernel, tuple(tiles), len(recvs)),
        grid_spec=pltpu.PrefetchScalarGridSpec(
            num_scalar_prefetch=1,
            grid=(1,),
            in_specs=[hbm] * (len(recvs) + 1),
            out_specs=hbm,
            scratch_shapes=[pltpu.VMEM((slots, half, BN), jnp.float32), pltpu.SemaphoreType.DMA((slots,)), pltpu.SemaphoreType.DMA((slots,))],
        ),
        out_shape=jax.ShapeDtypeStruct(prev.shape, prev.dtype),
        input_output_aliases={1 + len(recvs): 0},
        compiler_params=pltpu.CompilerParams(vmem_limit_bytes=VMEM_LIMIT, dimension_semantics=('arbitrary',)),
        cost_estimate=pl.CostEstimate(flops=40 * half * BN * len(tiles), bytes_accessed=8 * half * BN * len(tiles), transcendentals=0),
        name='place_pass',
    )(bases, *[r for r, _, _ in recvs], prev)


def solution(mesh):
    tp_size, cp_size, dp_size = mesh.shape['tp'], mesh.shape['cp'], mesh.shape['dp']
    from_next_pairs = [(cp_idx + 1, cp_idx) for cp_idx in range(cp_size - 1)]
    from_prev_pairs = [(cp_idx - 1, cp_idx) for cp_idx in range(1, cp_size)]
    tp_swap = [(t, 1 - t) for t in range(tp_size)]
    cp_swap = [(c, 1 - c) for c in range(cp_size)]
    core_swap = [(d, d ^ 1) for d in range(dp_size)]
    x_swap = [(d, d ^ 2) for d in range(dp_size)]

    def local_fn(hidden, tokens, seq_lens, norm_gain, w_head):
        n_seqs, local_len, depth = hidden.shape
        rows = n_seqs * local_len
        seg_len = local_len // 2
        vocab_local = w_head.shape[1]
        cp_rank = lax.axis_index('cp')
        tp_rank = lax.axis_index('tp')
        dp_rank = lax.axis_index('dp')
        core = dp_rank % 2

        def swap(v, axis, pairs):
            return lax.ppermute(v, axis, pairs)

        h_f32 = hidden.reshape(rows, depth).astype(jnp.float32)
        inv_rms = lax.rsqrt(jnp.mean(h_f32 * h_f32, axis=-1, keepdims=True) + NORM_EPS)
        x_hat = h_f32 * inv_rms
        x_norm = (x_hat * norm_gain).astype(jnp.bfloat16)
        x_all = lax.all_gather(x_hat, ('cp', 'dp'), tiled=True)

        heads = lax.optimization_barrier((tokens[:, :1], tokens[:, seg_len:seg_len + 1]))
        next_first = swap(heads[0], 'cp', from_next_pairs)
        prev_second = swap(heads[1], 'cp', from_prev_pairs)
        first_end = jnp.where(cp_rank == cp_size - 1, heads[1], next_first)
        shifted = jnp.concatenate([tokens[:, 1:], tokens[:, :1]], axis=1)
        column = jnp.arange(local_len)[None]
        labels = jnp.where(column == seg_len - 1, first_end, jnp.where(column == local_len - 1, prev_second, shifted))
        seg_pos = jnp.arange(seg_len)
        positions = jnp.concatenate([cp_rank * seg_len + seg_pos, (2 * cp_size - 1 - cp_rank) * seg_len + seg_pos])
        valid_mask = (positions[None, :] + 1 < seq_lens[:, None]).astype(jnp.float32)

        len_sum = jnp.full((128,), jnp.sum(seq_lens - 1).astype(jnp.float32))
        len_parts = [swap(len_sum, 'dp', [(d, d ^ k) for d in range(dp_size)]) for k in range(1, dp_size)]

        z, m_lane, s_lane = logits_pass(x_norm, w_head, 2048)
        valid_count = functools.reduce(jnp.add, len_parts, len_sum)[0]
        m_loc = jnp.max(m_lane, axis=-1)
        s_loc = jnp.sum(s_lane * jnp.exp(m_lane - m_loc[:, None]), axis=-1)
        m_far, s_far = swap(jnp.stack([m_loc, s_loc]), 'tp', tp_swap)
        glob_max = jnp.maximum(m_loc, m_far)
        log_norm = glob_max + jnp.log(s_loc * jnp.exp(m_loc - glob_max) + s_far * jnp.exp(m_far - glob_max))
        tok_scale = valid_mask.reshape(rows) / valid_count
        local_lab = labels.reshape(rows) - tp_rank * vocab_local

        stats = jnp.stack([log_norm, local_lab.astype(jnp.float32), tok_scale])
        n_group = cp_size * dp_size
        dx_rows = (log_norm, tok_scale, local_lab)
        stats, dx_rows = lax.optimization_barrier((stats, dx_rows))
        far_stats = [swap(stats, ('cp', 'dp'), [(d, d ^ k) for d in range(n_group)]) for k in range(1, n_group)]
        stats_all = [stats, *far_stats]
        mine = cp_rank * dp_size + dp_rank

        def wide(v):
            return jnp.broadcast_to(v.reshape(-1, 1), (v.size, 128))

        dx_part, t_lane = dx_pass(z, w_head, *[wide(v) for v in dx_rows], 1024)
        t_part = jnp.sum(t_lane, axis=-1)
        dx_part, x_all = lax.optimization_barrier((dx_part, x_all))
        xn_all, xt_all, lse_w, scale_w, lab_w = prep_pass(mine[None].astype(jnp.int32), x_all, norm_gain, stats_all)
        dx_norm = dx_part + swap(dx_part, 'tp', tp_swap)
        target_logit = t_part + swap(t_part, 'tp', tp_swap)
        tok_loss = (log_norm - target_logit).reshape(n_seqs, local_len) * valid_mask

        sums = jnp.concatenate([jnp.sum(dx_norm * x_hat, axis=0), jnp.full((128,), jnp.sum(tok_loss))])
        sums = sums + swap(sums, 'dp', core_swap)
        sums = sums + swap(sums, 'dp', x_swap)
        sums = sums + swap(sums, 'cp', cp_swap)
        d_gain = sums[:depth]
        loss_mean = sums[depth] / valid_count
        dx_hat = dx_norm * norm_gain
        d_hidden = (inv_rms * (dx_hat - x_hat * jnp.mean(dx_hat * x_hat, axis=-1, keepdims=True))).astype(jnp.bfloat16)

        n_blocks = vocab_local // BN
        shared, common = SHARED_SIZES, COMMON_SIZES
        n_shared, n_common = sum(shared), sum(common)
        assert 4 * n_shared + 2 * n_common == n_blocks
        role = (dp_rank // 2 + cp_rank) % 2

        table, entries = [], {}

        def add(name, const, by_role, by_core):
            entries[name] = len(table)
            table.append((const, by_role, by_core))

        for k in range(len(shared)):
            first = sum(shared[:k])
            add(('mine', k), first, 2 * n_shared, n_shared)
            add(('core', k), first + n_shared, 2 * n_shared, -n_shared)
            add(('chip', k), first + 2 * n_shared, -2 * n_shared, n_shared)
            add(('pass', k), first + 3 * n_shared, -2 * n_shared, -n_shared)
        for k in range(len(common)):
            first = 4 * n_shared + sum(common[:k])
            add(('all', k), first, 0, n_common)
            add(('core_all', k), first + n_common, 0, -n_common)
        parts = np.asarray(table, np.int32).T
        bases = (parts[0] + parts[1] * role + parts[2] * core).astype(jnp.int32)

        lower = N_CHUNK // 2
        out = None

        def run(n, entry, halves, arrived):
            return dw_pass(n, entries[entry], bases, halves, arrived, out, w_head, xn_all, xt_all, lse_w, scale_w, lab_w)

        from_core, from_chip, passed_on, from_core_common = {}, {}, {}, {}

        def share(k, send_x, send_y):
            where = entries['core', k]
            from_core[k] = [(swap(send_x, 'dp', core_swap), 0, where), (swap(send_y, 'dp', core_swap), lower, where)]
            where = entries['chip', k]
            from_chip[k] = [(swap(send_x, 'dp', x_swap), 0, where), (swap(send_y, 'cp', cp_swap), lower, where)]

        def pass_on(k):
            nonlocal out
            where = entries['chip', k]
            up, low, out = lax.optimization_barrier((from_chip[k][0][0], from_chip[k][1][0], out))
            from_chip[k] = [(up, 0, where), (low, lower, where)]
            where = entries['pass', k]
            passed_on[k] = [(swap(up, 'dp', core_swap), 0, where), (swap(low, 'dp', core_swap), lower, where)]

        def share_common(k, send):
            from_core_common[k] = [(swap(send, 'dp', core_swap), 0, entries['core_all', k])]

        for k in range(2):
            out, *sent = run(shared[k], ('mine', k), True, [])
            share(k, *sent)
        out, send = run(common[0], ('all', 0), False, from_core[0])
        share_common(0, send)
        pass_on(0)
        out, send = run(common[1], ('all', 1), False, from_core[1] + from_chip[0])
        share_common(1, send)
        pass_on(1)
        out, send = run(common[2], ('all', 2), False, passed_on[0] + from_core_common[0] + from_chip[1])
        share_common(2, send)
        out = place_pass(passed_on[1] + from_core_common[1], bases, out)
        d_head = place_pass(from_core_common[2], bases, out)
        return tok_loss, loss_mean, d_hidden.reshape(hidden.shape), d_gain, d_head

    return jax.shard_map(local_fn, mesh=mesh, in_specs=(P('dp', 'cp', None), P('dp', 'cp'), P('dp'), P(None), P(None, 'tp')), out_specs=(P('dp', 'cp'), P(), P('dp', 'cp', None), P(None), P(None, 'tp')), check_vma=False)
```

```python
import functools

import jax
import jax.numpy as jnp
import numpy as np
from jax import lax
from jax.experimental import pallas as pl
from jax.experimental.pallas import tpu as pltpu
from jax.sharding import PartitionSpec as P


NORM_EPS = 1e-5
BN = 512
N_CHUNK = 4
SHARED_SIZES = (2, 4)
COMMON_SIZES = (5, 4, 3)
VMEM_LIMIT = 67043328


def logits_kernel(x_ref, w_ref, z_ref, m_ref, s_ref):
    @pl.when(pl.program_id(0) == 0)
    def _():
        m_ref[...] = jnp.full_like(m_ref, -jnp.inf)
        s_ref[...] = jnp.zeros_like(s_ref)

    sub = 512
    for j in range(w_ref.shape[1] // sub):
        z = jnp.dot(x_ref[...], w_ref[:, j * sub:(j + 1) * sub], preferred_element_type=jnp.float32)
        z_ref[:, j * sub:(j + 1) * sub] = z
        parts = [z[:, k * 128:(k + 1) * 128] for k in range(sub // 128)]
        m_old = m_ref[...]
        m_new = functools.reduce(jnp.maximum, parts, m_old)
        acc = s_ref[...] * jnp.exp(m_old - m_new)
        for part in parts:
            acc = acc + jnp.exp(part - m_new)
        s_ref[...] = acc
        m_ref[...] = m_new


def logits_pass(x_norm, w_head, block):
    rows, depth = x_norm.shape
    vocab = w_head.shape[1]
    return pl.pallas_call(
        logits_kernel,
        grid=(vocab // block,),
        in_specs=[pl.BlockSpec((rows, depth), lambda i: (0, 0)), pl.BlockSpec((depth, block), lambda i: (0, i))],
        out_specs=[pl.BlockSpec((rows, block), lambda i: (0, i)), pl.BlockSpec((rows, 128), lambda i: (0, 0)), pl.BlockSpec((rows, 128), lambda i: (0, 0))],
        out_shape=[jax.ShapeDtypeStruct((rows, vocab), jnp.float32), jax.ShapeDtypeStruct((rows, 128), jnp.float32), jax.ShapeDtypeStruct((rows, 128), jnp.float32)],
        compiler_params=pltpu.CompilerParams(vmem_limit_bytes=VMEM_LIMIT, dimension_semantics=('arbitrary',)),
        cost_estimate=pl.CostEstimate(flops=2 * rows * depth * vocab, bytes_accessed=vocab * (depth * 2 + rows * 4), transcendentals=rows * vocab),
        name='logits_pass',
    )(x_norm, w_head)


def dx_kernel(n_blocks, z_ref, w_ref, lse_ref, scale_ref, lab_ref, dx_ref, t_ref, dz_buf):
    i = pl.program_id(0)
    rows, block = z_ref.shape

    @pl.when(i == 0)
    def _():
        dx_ref[...] = jnp.zeros_like(dx_ref)
        t_ref[...] = jnp.zeros_like(t_ref)
        dz_buf[1] = jnp.zeros(dz_buf.shape[1:], dz_buf.dtype)

    now, before = lax.rem(i, 2), lax.rem(i + 1, 2)
    lse, scale, lab = lse_ref[...], scale_ref[...], lab_ref[...]
    lab = jnp.where(i < n_blocks, lab, -1)
    lane = lax.broadcasted_iota(jnp.int32, (rows, 128), 1)
    first = i * block
    n_sub = 4
    width = dx_ref.shape[1] // n_sub
    for j in range(n_sub):
        dx_ref[:, j * width:(j + 1) * width] += lax.dot_general(dz_buf[before], w_ref[j * width:(j + 1) * width, :], (((1,), (1,)), ((), ())), preferred_element_type=jnp.float32)
    hit_sum = t_ref[...]
    for k in range(block // 128):
        z = z_ref[:, k * 128:(k + 1) * 128]
        hit = lab == lane + (first + k * 128)
        hit_sum = hit_sum + jnp.where(hit, z, 0.0)
        prob = jnp.exp(z - lse)
        dz_buf[now, :, k * 128:(k + 1) * 128] = (jnp.where(hit, prob - 1.0, prob) * scale).astype(jnp.bfloat16)
    t_ref[...] = hit_sum


def dx_pass(z, w_head, lse, scale, lab, block):
    rows, vocab = z.shape
    depth = w_head.shape[0]
    n_blocks = vocab // block
    row_spec = pl.BlockSpec((rows, 128), lambda i: (0, 0))
    return pl.pallas_call(
        functools.partial(dx_kernel, n_blocks),
        grid=(n_blocks + 1,),
        in_specs=[pl.BlockSpec((rows, block), lambda i: (0, jnp.minimum(i, n_blocks - 1))), pl.BlockSpec((depth, block), lambda i: (0, jnp.maximum(i - 1, 0))), row_spec, row_spec, row_spec],
        out_specs=[pl.BlockSpec((rows, depth), lambda i: (0, 0)), row_spec],
        out_shape=[jax.ShapeDtypeStruct((rows, depth), jnp.float32), jax.ShapeDtypeStruct((rows, 128), jnp.float32)],
        scratch_shapes=[pltpu.VMEM((2, rows, block), jnp.bfloat16)],
        compiler_params=pltpu.CompilerParams(vmem_limit_bytes=VMEM_LIMIT, dimension_semantics=('arbitrary',)),
        cost_estimate=pl.CostEstimate(flops=2 * rows * depth * vocab, bytes_accessed=vocab * (depth * 2 + rows * 4), transcendentals=rows * vocab),
        name='dx_pass',
    )(z, w_head, lse, scale, lab)


def prep_kernel(mine_ref, x_ref, g_ref, *refs):
    xn_ref, xt_ref, lse_out, scale_out, lab_out = refs[-5:]
    source = jnp.bitwise_xor(mine_ref[0], pl.program_id(0))
    stats = refs[0][...]
    for k in range(1, len(refs) - 5):
        stats = jnp.where(source == k, refs[k][...], stats)
    xn = (x_ref[...] * g_ref[...]).astype(jnp.bfloat16)
    xn_ref[...] = xn
    xt_ref[...] = xn.T
    block = x_ref.shape[0]

    def wide(k):
        return jnp.broadcast_to(stats[k:k + 1, :], (128, block)).T

    lse_out[...] = wide(0)
    scale_out[...] = wide(2)
    lab_out[...] = wide(1).astype(jnp.int32)


def prep_pass(mine, x_all, norm_gain, stats):
    tokens, depth = x_all.shape
    n = len(stats)
    n_stats, block = stats[0].shape
    wide_spec = pl.BlockSpec((block, 128), lambda i, mine: (i, 0))
    return pl.pallas_call(
        prep_kernel,
        grid_spec=pltpu.PrefetchScalarGridSpec(
            num_scalar_prefetch=1,
            grid=(n,),
            in_specs=[pl.BlockSpec((block, depth), lambda i, mine: (i, 0)), pl.BlockSpec((1, depth), lambda i, mine: (0, 0)), *[pl.BlockSpec((n_stats, block), lambda i, mine: (0, 0))] * n],
            out_specs=[pl.BlockSpec((block, depth), lambda i, mine: (i, 0)), pl.BlockSpec((depth, block), lambda i, mine: (0, i)), wide_spec, wide_spec, wide_spec],
        ),
        out_shape=[jax.ShapeDtypeStruct((tokens, depth), jnp.bfloat16), jax.ShapeDtypeStruct((depth, tokens), jnp.bfloat16)] + [jax.ShapeDtypeStruct((tokens, 128), t) for t in (jnp.float32, jnp.float32, jnp.int32)],
        compiler_params=pltpu.CompilerParams(vmem_limit_bytes=VMEM_LIMIT, dimension_semantics=('arbitrary',)),
        cost_estimate=pl.CostEstimate(flops=8 * tokens * depth, bytes_accessed=8 * tokens * depth, transcendentals=0),
        name='prep_pass',
    )(mine, x_all, norm_gain[None], *stats)


def dw_kernel(n, entry, halves, n_recv, lanes, has_prev, bases_ref, w_ref, xn_hbm, xt_hbm, lse_hbm, scale_hbm, lab_hbm, *rest):
    recvs = rest[:n_recv]
    rest = rest[n_recv + (1 if has_prev else 0):]
    out_ref = rest[0]
    n_sends = 2 if halves else 1
    sends = rest[1:1 + n_sends]
    xn, xt, lse_v, scale_v, lab_v, dz_buf, o_buf, r_buf, in_sem, st_sem, out_sem, send_sem, rin_sem, rout_sem = rest[1 + n_sends:]
    i = pl.program_id(0)
    tokens, depth = xn.shape
    tok = tokens // N_CHUNK
    row = depth // N_CHUNK
    now, before = lax.rem(i, 2), lax.rem(i + 1, 2)

    def xn_copy(t):
        part = pl.ds(pl.multiple_of(t * tok, tok), tok)
        return pltpu.make_async_copy(xn_hbm.at[part, :], xn.at[part, :], in_sem.at[t])

    def xt_copy(t):
        part = pl.ds(pl.multiple_of(t * row, row), row)
        return pltpu.make_async_copy(xt_hbm.at[part, :], xt.at[part, :], in_sem.at[N_CHUNK + t])

    def stat_copies(t):
        part = pl.ds(pl.multiple_of(t * tok, tok), tok)
        return [pltpu.make_async_copy(src.at[part, :], dst.at[part, :], st_sem.at[k, t]) for k, (src, dst) in enumerate(((lse_hbm, lse_v), (scale_hbm, scale_v), (lab_hbm, lab_v)))]

    def tile(ref, r, block):
        return ref.at[pl.ds(pl.multiple_of(r * row, row), row), pl.ds(pl.multiple_of(block * BN, BN), BN)]

    def out_copy(step, t, slot):
        return pltpu.make_async_copy(o_buf.at[slot], tile(out_ref, t, bases_ref[entry] + step), out_sem.at[slot])

    def send_copy(k, r, block, slot):
        return pltpu.make_async_copy(o_buf.at[slot], tile(sends[k], r, block), send_sem.at[slot])

    def finish_out(slot):
        out_copy(0, 0, slot).wait()
        send_copy(0, 0, 0, slot).wait()

    def rin_copy(lane, ref, r, block, slot):
        return pltpu.make_async_copy(tile(ref, r, block), r_buf.at[slot, lane], rin_sem.at[slot, lane])

    def rout_copy(lane, r, block, slot):
        return pltpu.make_async_copy(r_buf.at[slot, lane], tile(out_ref, r, block), rout_sem.at[slot, lane])

    def move_tiles(t):
        v = i * N_CHUNK + t
        slot, other = lax.rem(v, 2), lax.rem(v + 1, 2)
        for lane, entries in enumerate(lanes):
            total = sum(entry[4] for entry in entries)
            at = 0
            for k, where, first_row, u0, count, per_block in entries:
                @pl.when((v >= at + 1) & (v < at + 1 + count))
                def _(at=at, where=where, first_row=first_row, u0=u0, per_block=per_block):
                    u = v - 1 - at + u0
                    rin_copy(lane, recvs[0], 0, 0, other).wait()
                    rout_copy(lane, first_row + lax.rem(u, per_block), bases_ref[where] + u // per_block, other).start()

                at += count

            @pl.when((v >= 2) & (v < total + 2))
            def _():
                rout_copy(lane, 0, 0, slot).wait()

            at = 0
            for k, where, first_row, u0, count, per_block in entries:
                @pl.when((v >= at) & (v < at + count))
                def _(at=at, k=k, u0=u0, per_block=per_block):
                    u = v - at + u0
                    rin_copy(lane, recvs[k], lax.rem(u, per_block), u // per_block, slot).start()

                at += count

    def make_dz(t):
        part = pl.ds(pl.multiple_of(t * tok, tok), tok)
        z = jnp.dot(xn[part, :], w_ref[...], preferred_element_type=jnp.float32)
        lse, scale, lab = lse_v[part, :], scale_v[part, :], lab_v[part, :]
        lane_id = lax.broadcasted_iota(jnp.int32, (tok, 128), 1)
        first = (bases_ref[entry] + jnp.minimum(i, n - 1)) * BN
        for k in range(BN // 128):
            prob = jnp.exp(z[:, k * 128:(k + 1) * 128] - lse)
            hit = lab == lane_id + (first + k * 128)
            dz_buf[now, part, k * 128:(k + 1) * 128] = (jnp.where(hit, prob - 1.0, prob) * scale).astype(jnp.bfloat16)

    def make_dw(t):
        part = pl.ds(pl.multiple_of(t * row, row), row)
        o_buf[lax.rem(t, 2)] = jnp.dot(xt[part, :], dz_buf[before], preferred_element_type=jnp.float32)

    def flush(t):
        slot = lax.rem(t, 2)
        out_copy(i - 1, t, slot).start()
        if halves:
            @pl.when(t < N_CHUNK // 2)
            def _():
                send_copy(0, t, i - 1, slot).start()

            @pl.when(t >= N_CHUNK // 2)
            def _():
                send_copy(1, t - N_CHUNK // 2, i - 1, slot).start()
        else:
            send_copy(0, t, i - 1, slot).start()

    def loop(do_dz, do_dw):
        def body(t, carry):
            move_tiles(t)
            if do_dw:
                @pl.when((i > 1) | (t > 1))
                def _():
                    finish_out(lax.rem(t, 2))

                @pl.when(i == 1)
                def _():
                    xt_copy(t).wait()
            else:
                xn_copy(t).wait()
                for copy in stat_copies(t):
                    copy.wait()

                @pl.when(t + 2 < N_CHUNK)
                def _():
                    xn_copy(t + 2).start()
                    for copy in stat_copies(t + 2):
                        copy.start()

                xt_copy(t).start()
            if do_dw:
                make_dw(t)
            if do_dz:
                make_dz(t)
            if do_dw:
                flush(t)
            return carry

        lax.fori_loop(0, N_CHUNK, body, 0)

    @pl.when(i == 0)
    def _():
        for t in range(2):
            xn_copy(t).start()
            for copy in stat_copies(t):
                copy.start()
        loop(True, False)

    @pl.when((i > 0) & (i < n))
    def _():
        loop(True, True)

    @pl.when(i == n)
    def _():
        loop(False, True)
        finish_out(0)
        finish_out(1)


def plan_lanes(recvs, row, n):
    room = (n + 1) * N_CHUNK - 2
    lanes, left = [], 0
    for k, (array, first_row, where) in enumerate(recvs):
        per_block = array.shape[0] // row
        total = per_block * (array.shape[1] // BN)
        done = 0
        while done < total:
            if left == 0:
                lanes.append([])
                left = room
            take = min(left, total - done)
            lanes[-1].append((k, where, first_row, done, take, per_block))
            done += take
            left -= take
    return tuple(tuple(lane) for lane in lanes)


def dw_pass(n, entry, bases, halves, recvs, prev, w_head, xn, xt, lse, scale, lab):
    depth, vocab = w_head.shape
    tokens = xn.shape[0]
    row = depth // N_CHUNK
    hbm = pl.BlockSpec(memory_space=pl.ANY)
    operands = [w_head, xn, xt, lse, scale, lab, *[r for r, _, _ in recvs]]
    if prev is not None:
        operands.append(prev)
    lanes = plan_lanes(recvs, row, n)
    n_lanes = max(len(lanes), 1)
    send_rows = [depth // 2] * 2 if halves else [depth]
    out_shape = [jax.ShapeDtypeStruct((depth, vocab), jnp.float32)] + [jax.ShapeDtypeStruct((r, n * BN), jnp.float32) for r in send_rows]
    grid_spec = pltpu.PrefetchScalarGridSpec(
        num_scalar_prefetch=1,
        grid=(n + 1,),
        in_specs=[pl.BlockSpec((depth, BN), lambda i, bases: (0, bases[entry] + jnp.minimum(i, n - 1)))] + [hbm] * (len(operands) - 1),
        out_specs=[hbm] * len(out_shape),
        scratch_shapes=[
            pltpu.VMEM((tokens, depth), jnp.bfloat16),
            pltpu.VMEM((depth, tokens), jnp.bfloat16),
            pltpu.VMEM((tokens, 128), jnp.float32),
            pltpu.VMEM((tokens, 128), jnp.float32),
            pltpu.VMEM((tokens, 128), jnp.int32),
            pltpu.VMEM((2, tokens, BN), jnp.bfloat16),
            pltpu.VMEM((2, row, BN), jnp.float32),
            pltpu.VMEM((2, n_lanes, row, BN) if lanes else (2, 1, 8, 128), jnp.float32),
            pltpu.SemaphoreType.DMA((2 * N_CHUNK,)),
            pltpu.SemaphoreType.DMA((3, N_CHUNK)),
            pltpu.SemaphoreType.DMA((2,)),
            pltpu.SemaphoreType.DMA((2,)),
            pltpu.SemaphoreType.DMA((2, n_lanes)),
            pltpu.SemaphoreType.DMA((2, n_lanes)),
        ],
    )
    width = n * BN
    return pl.pallas_call(
        functools.partial(dw_kernel, n, entry, halves, len(recvs), lanes, prev is not None),
        grid_spec=grid_spec,
        out_shape=out_shape,
        input_output_aliases={} if prev is None else {1 + len(operands) - 1: 0},
        compiler_params=pltpu.CompilerParams(vmem_limit_bytes=VMEM_LIMIT, dimension_semantics=('arbitrary',)),
        cost_estimate=pl.CostEstimate(flops=4 * tokens * depth * width, bytes_accessed=depth * width * 10, transcendentals=tokens * width),
    )(bases, *operands)


def place_kernel(tiles, n_recv, bases_ref, *rest):
    recvs = rest[:n_recv]
    out_ref, buf, in_sem, out_sem = rest[n_recv + 1:]
    slots = buf.shape[0]

    def tile(ref, r, block):
        half = buf.shape[1]
        return ref.at[pl.ds(r * half, half), pl.ds(pl.multiple_of(block * BN, BN), BN)]

    def load(u):
        k, r, block, _, _ = tiles[u]
        return pltpu.make_async_copy(tile(recvs[k], r, block), buf.at[u % slots], in_sem.at[u % slots])

    def store(u):
        _, _, block, to_row, where = tiles[u]
        return pltpu.make_async_copy(buf.at[u % slots], tile(out_ref, to_row, bases_ref[where] + block), out_sem.at[u % slots])

    ahead = slots // 2
    n = len(tiles)
    for u in range(min(ahead, n)):
        load(u).start()
    for u in range(n):
        load(u).wait()
        store(u).start()
        if u + ahead < n:
            if u + ahead >= slots:
                store(u + ahead - slots).wait()
            load(u + ahead).start()
    for u in range(max(n - slots, 0), n):
        store(u).wait()


def place_pass(recvs, bases, prev):
    depth = prev.shape[0]
    half = depth // 2
    tiles = []
    for k, (array, first_row, where) in enumerate(recvs):
        for block in range(array.shape[1] // BN):
            for r in range(array.shape[0] // half):
                tiles.append((k, r, block, first_row // (N_CHUNK // 2) + r, where))
    hbm = pl.BlockSpec(memory_space=pl.ANY)
    slots = 12
    return pl.pallas_call(
        functools.partial(place_kernel, tuple(tiles), len(recvs)),
        grid_spec=pltpu.PrefetchScalarGridSpec(
            num_scalar_prefetch=1,
            grid=(1,),
            in_specs=[hbm] * (len(recvs) + 1),
            out_specs=hbm,
            scratch_shapes=[pltpu.VMEM((slots, half, BN), jnp.float32), pltpu.SemaphoreType.DMA((slots,)), pltpu.SemaphoreType.DMA((slots,))],
        ),
        out_shape=jax.ShapeDtypeStruct(prev.shape, prev.dtype),
        input_output_aliases={1 + len(recvs): 0},
        compiler_params=pltpu.CompilerParams(vmem_limit_bytes=VMEM_LIMIT, dimension_semantics=('arbitrary',)),
        cost_estimate=pl.CostEstimate(flops=40 * half * BN * len(tiles), bytes_accessed=8 * half * BN * len(tiles), transcendentals=0),
        name='place_pass',
    )(bases, *[r for r, _, _ in recvs], prev)


def solution(mesh):
    tp_size, cp_size, dp_size = mesh.shape['tp'], mesh.shape['cp'], mesh.shape['dp']
    from_next_pairs = [(cp_idx + 1, cp_idx) for cp_idx in range(cp_size - 1)]
    from_prev_pairs = [(cp_idx - 1, cp_idx) for cp_idx in range(1, cp_size)]
    tp_swap = [(t, 1 - t) for t in range(tp_size)]
    cp_swap = [(c, 1 - c) for c in range(cp_size)]
    core_swap = [(d, d ^ 1) for d in range(dp_size)]
    x_swap = [(d, d ^ 2) for d in range(dp_size)]

    def local_fn(hidden, tokens, seq_lens, norm_gain, w_head):
        n_seqs, local_len, depth = hidden.shape
        rows = n_seqs * local_len
        seg_len = local_len // 2
        vocab_local = w_head.shape[1]
        cp_rank = lax.axis_index('cp')
        tp_rank = lax.axis_index('tp')
        dp_rank = lax.axis_index('dp')
        core = dp_rank % 2

        def swap(v, axis, pairs):
            return lax.ppermute(v, axis, pairs)

        h_f32 = hidden.reshape(rows, depth).astype(jnp.float32)
        inv_rms = lax.rsqrt(jnp.mean(h_f32 * h_f32, axis=-1, keepdims=True) + NORM_EPS)
        x_hat = h_f32 * inv_rms
        x_norm = (x_hat * norm_gain).astype(jnp.bfloat16)
        x_all = lax.all_gather(x_hat, ('cp', 'dp'), tiled=True)

        heads = lax.optimization_barrier((tokens[:, :1], tokens[:, seg_len:seg_len + 1]))
        next_first = swap(heads[0], 'cp', from_next_pairs)
        prev_second = swap(heads[1], 'cp', from_prev_pairs)
        first_end = jnp.where(cp_rank == cp_size - 1, heads[1], next_first)
        shifted = jnp.concatenate([tokens[:, 1:], tokens[:, :1]], axis=1)
        column = jnp.arange(local_len)[None]
        labels = jnp.where(column == seg_len - 1, first_end, jnp.where(column == local_len - 1, prev_second, shifted))
        seg_pos = jnp.arange(seg_len)
        positions = jnp.concatenate([cp_rank * seg_len + seg_pos, (2 * cp_size - 1 - cp_rank) * seg_len + seg_pos])
        valid_mask = (positions[None, :] + 1 < seq_lens[:, None]).astype(jnp.float32)

        len_sum = jnp.full((128,), jnp.sum(seq_lens - 1).astype(jnp.float32))
        len_parts = [swap(len_sum, 'dp', [(d, d ^ k) for d in range(dp_size)]) for k in range(1, dp_size)]

        z, m_lane, s_lane = logits_pass(x_norm, w_head, 2048)
        valid_count = functools.reduce(jnp.add, len_parts, len_sum)[0]
        m_loc = jnp.max(m_lane, axis=-1)
        s_loc = jnp.sum(s_lane * jnp.exp(m_lane - m_loc[:, None]), axis=-1)
        m_far, s_far = swap(jnp.stack([m_loc, s_loc]), 'tp', tp_swap)
        glob_max = jnp.maximum(m_loc, m_far)
        log_norm = glob_max + jnp.log(s_loc * jnp.exp(m_loc - glob_max) + s_far * jnp.exp(m_far - glob_max))
        tok_scale = valid_mask.reshape(rows) / valid_count
        local_lab = labels.reshape(rows) - tp_rank * vocab_local

        stats = jnp.stack([log_norm, local_lab.astype(jnp.float32), tok_scale])
        n_group = cp_size * dp_size
        dx_rows = (log_norm, tok_scale, local_lab)
        stats, dx_rows = lax.optimization_barrier((stats, dx_rows))
        far_stats = [swap(stats, ('cp', 'dp'), [(d, d ^ k) for d in range(n_group)]) for k in range(1, n_group)]
        stats_all = [stats, *far_stats]
        mine = cp_rank * dp_size + dp_rank

        def wide(v):
            return jnp.broadcast_to(v.reshape(-1, 1), (v.size, 128))

        dx_part, t_lane = dx_pass(z, w_head, *[wide(v) for v in dx_rows], 1024)
        t_part = jnp.sum(t_lane, axis=-1)
        dx_part, x_all = lax.optimization_barrier((dx_part, x_all))
        xn_all, xt_all, lse_w, scale_w, lab_w = prep_pass(mine[None].astype(jnp.int32), x_all, norm_gain, stats_all)
        dx_norm = dx_part + swap(dx_part, 'tp', tp_swap)
        target_logit = t_part + swap(t_part, 'tp', tp_swap)
        tok_loss = (log_norm - target_logit).reshape(n_seqs, local_len) * valid_mask

        sums = jnp.concatenate([jnp.sum(dx_norm * x_hat, axis=0), jnp.full((128,), jnp.sum(tok_loss))])
        sums = sums + swap(sums, 'dp', core_swap)
        sums = sums + swap(sums, 'dp', x_swap)
        sums = sums + swap(sums, 'cp', cp_swap)
        d_gain = sums[:depth]
        loss_mean = sums[depth] / valid_count
        dx_hat = dx_norm * norm_gain
        d_hidden = (inv_rms * (dx_hat - x_hat * jnp.mean(dx_hat * x_hat, axis=-1, keepdims=True))).astype(jnp.bfloat16)

        n_blocks = vocab_local // BN
        shared, common = SHARED_SIZES, COMMON_SIZES
        n_shared, n_common = sum(shared), sum(common)
        assert 4 * n_shared + 2 * n_common == n_blocks
        role = (dp_rank // 2 + cp_rank) % 2

        table, entries = [], {}

        def add(name, const, by_role, by_core):
            entries[name] = len(table)
            table.append((const, by_role, by_core))

        for k in range(len(shared)):
            first = sum(shared[:k])
            add(('mine', k), first, 2 * n_shared, n_shared)
            add(('core', k), first + n_shared, 2 * n_shared, -n_shared)
            add(('chip', k), first + 2 * n_shared, -2 * n_shared, n_shared)
            add(('pass', k), first + 3 * n_shared, -2 * n_shared, -n_shared)
        for k in range(len(common)):
            first = 4 * n_shared + sum(common[:k])
            add(('all', k), first, 0, n_common)
            add(('core_all', k), first + n_common, 0, -n_common)
        parts = np.asarray(table, np.int32).T
        bases = (parts[0] + parts[1] * role + parts[2] * core).astype(jnp.int32)

        lower = N_CHUNK // 2
        out = None

        def run(n, entry, halves, arrived):
            return dw_pass(n, entries[entry], bases, halves, arrived, out, w_head, xn_all, xt_all, lse_w, scale_w, lab_w)

        from_core, from_chip, passed_on, from_core_common = {}, {}, {}, {}

        def share(k, send_x, send_y):
            where = entries['core', k]
            from_core[k] = [(swap(send_x, 'dp', core_swap), 0, where), (swap(send_y, 'dp', core_swap), lower, where)]
            where = entries['chip', k]
            from_chip[k] = [(swap(send_x, 'dp', x_swap), 0, where), (swap(send_y, 'cp', cp_swap), lower, where)]

        def pass_on(k):
            nonlocal out
            where = entries['chip', k]
            up, low, out = lax.optimization_barrier((from_chip[k][0][0], from_chip[k][1][0], out))
            from_chip[k] = [(up, 0, where), (low, lower, where)]
            where = entries['pass', k]
            passed_on[k] = [(swap(up, 'dp', core_swap), 0, where), (swap(low, 'dp', core_swap), lower, where)]

        def share_common(k, send):
            from_core_common[k] = [(swap(send, 'dp', core_swap), 0, entries['core_all', k])]

        for k in range(2):
            out, *sent = run(shared[k], ('mine', k), True, [])
            share(k, *sent)
        out, send = run(common[0], ('all', 0), False, from_core[0])
        share_common(0, send)
        pass_on(0)
        out, send = run(common[1], ('all', 1), False, from_core[1] + from_chip[0])
        share_common(1, send)
        pass_on(1)
        out, send = run(common[2], ('all', 2), False, passed_on[0] + from_core_common[0] + from_chip[1])
        share_common(2, send)
        out = place_pass(passed_on[1] + from_core_common[1], bases, out)
        d_head = place_pass(from_core_common[2], bases, out)
        return tok_loss, loss_mean, d_hidden.reshape(hidden.shape), d_gain, d_head

    return jax.shard_map(local_fn, mesh=mesh, in_specs=(P('dp', 'cp', None), P('dp', 'cp'), P('dp'), P(None), P(None, 'tp')), out_specs=(P('dp', 'cp'), P(), P('dp', 'cp', None), P(None), P(None, 'tp')), check_vma=False)
```
